256 devices in a mesh: groups: 2 (over y), expert: 16 (over z), hidden: 8 (over x, core).
Axes of the slice: x: 4, y: 2, z: 16, core: 2. Of those that a mesh axis runs over, the one named last changes fastest.
The devices are a block of a 4x16x16 slice.
Arguments:
- tokens: bfloat16 [256, 196, 1024], P(('groups', 'expert', 'hidden')), parts along dimension 0, may hold values from -40 to 40
- slot_params: bfloat16 [2048, 64], P('groups'), parts along dimension 0, may hold values from -0.75 to 0.75
- expert_up: bfloat16 [128, 1024, 4096], P(('groups', 'expert'), None, 'hidden'), parts along dimension 0, may hold values from -0.1875 to 0.1875
- expert_down: bfloat16 [128, 4096, 1024], P(('groups', 'expert'), 'hidden'), parts along dimension 0, may hold values from -0.09375 to 0.09375
- cotangent: bfloat16 [256, 196, 1024], P(('groups', 'expert', 'hidden')), parts along dimension 0, may hold values from -6 to 6
Outputs:
- mixed: bfloat16 [256, 196, 1024], P(('groups', 'expert', 'hidden')), parts along dimension 0
- d_tokens: bfloat16 [256, 196, 1024], P(('groups', 'expert', 'hidden')), parts along dimension 0
- d_slot_params: float32 [2048, 64], P('groups'), parts along dimension 0
The draws below stay inside these ranges and needn't reach their ends.
There are 2 independent parts, one for each index of `groups`. The reference program is written for one: setup_inputs(seed, part) draws one part's arguments, and reference() takes and returns one part's arrays. A program takes and returns all parts, laid end to end along the dimension named above; each array names one. Nothing has to cross between parts.
All inputs are finite; a program needn't handle non-finite values.
Results may differ from the reference program's by a relative error of at most 0.0077.
Values may be sent and summed in bfloat16 or wider, within the bound.
A program may use at most 64 MiB of HBM per device.

```python
import math
import jax
import jax.numpy as jnp
from jax import lax

D = 1024
FF = 4096
TOKENS = 196
SPE = 1
EXPERTS = 64
SLOTS = 64
IMAGES = 128


def shared_draw(key):
    base_normal = jax.random.normal(jax.random.fold_in(key, 11), (D, SLOTS), jnp.float32)
    chosen = jax.random.permutation(jax.random.fold_in(key, 12), SLOTS)[:6]
    picked = base_normal[:, chosen]
    columns = []
    for column_idx in range(6):
        vector = picked[:, column_idx]
        for earlier in columns:
            vector = vector - jnp.dot(earlier, vector, precision=lax.Precision.HIGHEST) * earlier
        columns.append(vector / jnp.sqrt(jnp.sum(vector * vector)))
    return base_normal


def draw_slot_params(key, part):
    base_normal = shared_draw(key)
    values = base_normal * (3.0 / math.sqrt(D))
    return jnp.clip(values, -0.75, 0.75).astype(jnp.bfloat16)


def draw_tokens(key, part):
    values = jax.random.normal(jax.random.fold_in(key, 21), (IMAGES, TOKENS, D), jnp.float32)
    return jnp.clip(values, -40.0, 40.0).astype(jnp.bfloat16)


def block_levels(stream_key, extent, split, smallest, largest):
    def one(position, blocks):
        draws = jax.random.uniform(jax.random.fold_in(jax.random.fold_in(stream_key, 6), position), (blocks,), jnp.float32, smallest / len(split), largest / len(split))
        return jnp.repeat(jnp.exp(draws), extent[position] // blocks).reshape((-1,) + (1,) * (len(extent) - position - 1))

    loudness = one(*split[0])
    for cut in split[1:]:
        loudness = loudness * one(*cut)
    return loudness


def normal_values(own_key, shape, deviation, bound, split=(), held_as=jnp.bfloat16):
    values = jax.random.normal(own_key, shape, jnp.float32) * deviation
    if len(split) > 0:
        values = block_levels(own_key, shape, split, -0.22, 0.18) * values
    return jnp.clip(values, min=-bound, max=bound).astype(held_as)


def setup_inputs(seed: int = 0, part: int = 0) -> dict:
    arg_keys = jax.random.split(jax.random.key(seed), 6)
    part_splits = jax.random.split(jax.random.fold_in(arg_keys[5], part), 6)
    return {
        "tokens": draw_tokens(jax.random.fold_in(jax.random.fold_in(arg_keys[5], part), 71), part),
        "slot_params": draw_slot_params(jax.random.fold_in(jax.random.fold_in(arg_keys[5], part), 71), part),
        "expert_up": normal_values(part_splits[2], (EXPERTS, D, FF), D ** -0.5, 0.1875, ((0, 16), (2, 8))),
        "expert_down": normal_values(part_splits[3], (EXPERTS, FF, D), FF ** -0.5, 0.09375, ((0, 16), (1, 8))),
        "cotangent": normal_values(part_splits[4], (IMAGES, TOKENS, D), 1.0, 6.0, ((0, 128),)),
    }


inv_root_two = 0.7071067811865476
inv_root_tau = 0.3989422804014327


def gelu_exact(value):
    return 0.5 * value * (1.0 + lax.erf(value * inv_root_two))


def gelu_slope(value):
    return 0.5 * (1.0 + lax.erf(value * inv_root_two)) + value * jnp.exp(-0.5 * value * value) * inv_root_tau


def rounded(value):
    return lax.optimization_barrier(value.astype(jnp.bfloat16)).astype(jnp.float32)


def reference(tokens, slot_params, expert_up, expert_down, cotangent):
    tokens_wide = tokens.astype(jnp.float32)
    params_wide = slot_params.astype(jnp.float32)
    grad_wide = cotangent.astype(jnp.float32)
    logits = jnp.einsum("imd,ds->ims", tokens_wide, params_wide)
    dispatch = jax.nn.softmax(logits, axis=1)
    combine = jax.nn.softmax(logits, axis=2)
    dispatch_half = rounded(dispatch)
    combine_half = rounded(combine)
    slots_in = rounded(jnp.einsum("ims,imd->isd", dispatch_half, tokens_wide))
    grouped_in = jnp.moveaxis(slots_in.reshape(IMAGES, EXPERTS, SPE, D), 1, 0)

    def forward_expert(bundle):
        row_block, up_matrix, down_matrix = bundle
        pre_act = jnp.einsum("isd,df->isf", row_block, up_matrix.astype(jnp.float32))
        activated = rounded(gelu_exact(pre_act))
        return rounded(jnp.einsum("isf,fd->isd", activated, down_matrix.astype(jnp.float32)))

    slots_out = lax.map(forward_expert, (grouped_in, expert_up, expert_down))
    slots_out = jnp.moveaxis(slots_out, 0, 1).reshape(IMAGES, SLOTS, D)
    mixed = jnp.einsum("ims,isd->imd", combine_half, slots_out)
    d_combine = jnp.einsum("imd,isd->ims", grad_wide, slots_out)
    d_slots_out = rounded(jnp.einsum("ims,imd->isd", combine_half, grad_wide))
    grouped_grad = jnp.moveaxis(d_slots_out.reshape(IMAGES, EXPERTS, SPE, D), 1, 0)

    def backward_expert(bundle):
        row_block, grad_block, up_matrix, down_matrix = bundle
        up_wide = up_matrix.astype(jnp.float32)
        pre_act = jnp.einsum("isd,df->isf", row_block, up_wide)
        slope_in = jnp.einsum("isd,fd->isf", grad_block, down_matrix.astype(jnp.float32))
        d_pre = rounded(slope_in * gelu_slope(pre_act))
        return rounded(jnp.einsum("isf,df->isd", d_pre, up_wide))

    d_slots_in = lax.map(backward_expert, (grouped_in, grouped_grad, expert_up, expert_down))
    d_slots_in = jnp.moveaxis(d_slots_in, 0, 1).reshape(IMAGES, SLOTS, D)
    d_dispatch = jnp.einsum("imd,isd->ims", tokens_wide, d_slots_in)
    grad_combine = rounded(combine * (d_combine - jnp.sum(combine * d_combine, axis=2, keepdims=True)))
    grad_dispatch = rounded(dispatch * (d_dispatch - jnp.sum(dispatch * d_dispatch, axis=1, keepdims=True)))
    d_tokens = jnp.einsum("ims,isd->imd", dispatch_half, d_slots_in)
    d_tokens = d_tokens + jnp.einsum("ims,ds->imd", grad_combine, params_wide)
    d_tokens = d_tokens + jnp.einsum("ims,ds->imd", grad_dispatch, params_wide)
    d_slot_params = jnp.einsum("imd,ims->ds", tokens_wide, grad_combine) + jnp.einsum("imd,ims->ds", tokens_wide, grad_dispatch)
    return mixed.astype(jnp.bfloat16), d_tokens.astype(jnp.bfloat16), d_slot_params.astype(jnp.float32)
```

```python
import functools
import types

import jax
import jax.numpy as jnp
from jax import lax
from jax.experimental import pallas as pl
from jax.experimental.pallas import tpu as pltpu
from jax.sharding import PartitionSpec as P

MESH = pl.DeviceIdType.MESH
BF16 = jnp.bfloat16
F32 = jnp.float32
LANES = 128
ROOT_HALF = 0.7071067811865476
ROOT_TAU = 0.3989422804014327
SPAN = 4

NT = (((1,), (1,)), ((), ()))
NN = (((1,), (0,)), ((), ()))


def dot(a, b, dims=NN):
    return lax.dot_general(a, b, dims, preferred_element_type=F32)


def gelu_exact(value):
    return 0.5 * value * (1.0 + lax.erf(value * ROOT_HALF))


def gelu_slope(value):
    return 0.5 * (1.0 + lax.erf(value * ROOT_HALF)) + value * jnp.exp(-0.5 * value * value) * ROOT_TAU


def scratch_plan(E, H, J, T, TP, S, D, FF):
    X, C = H // 2, D // LANES
    msg = J * C
    vm, dma = pltpu.VMEM, pltpu.SemaphoreType.DMA
    return dict(
        tok=vm((TP, D), BF16),
        cot=vm((TP, D), BF16),
        up=vm((J, D, FF), BF16),
        down=vm((J, FF, D), BF16),
        stage=vm((S * C, LANES), F32),
        a_send=vm((2, E, msg, LANES), BF16),
        a_recv=vm((2, E, msg, LANES), BF16),
        g=vm((2, J, H, E, D), BF16),
        pre=vm((J, H * E, FF), F32),
        part=vm((2, J, H, E, D), F32),
        d_send=vm((2, X, 2, J // 2, E, D), BF16),
        d_recv=vm((2, X, 2, J // 2, E, D), BF16),
        r1_send=vm((2, 2, J // 2, E, D), BF16),
        r1_recv=vm((2, 2, J // 2, E, D), BF16),
        r2_send=vm((2, 2, 2, J // 2, E, D), BF16),
        r2_recv=vm((2, 2, 2, J // 2, E, D), BF16),
        b_send=vm((2, E, msg, LANES), BF16),
        b_recv=vm((2, E, msg, LANES), BF16),
        slots=vm((2, S, D), BF16),
        comb=vm((TP, S), F32),
        comb_t=vm((S, TP), F32),
        disp=vm((TP, S), F32),
        disp_t=vm((S, TP), F32),
        grad_c=vm((TP, S), BF16),
        dsp_c=vm((S, D), F32),
        c_send=vm((H, S, LANES), BF16),
        c_own=vm((H, S, LANES), F32),
        c_recv=vm((H, S, LANES), BF16),
        n_all=vm((SPAN, S, LANES), BF16),
        n_send=vm((S, LANES), BF16),
        w_all=vm((E // SPAN, S, LANES), BF16),
        w_send=vm((S, LANES), BF16),
        f_all=vm((H, S, LANES), BF16),
        f_send=vm((S, LANES), BF16),
        in_sem=dma((2,)),
        a_ss=dma((2,)),
        a_rs=dma((2,)),
        g_ss=dma((2,)),
        g_rs=dma((2, 7)),
        d_ss=dma((2,)),
        d_rs=dma((2, X, 2)),
        r1_ss=dma((2,)),
        r1_rs=dma((2, 2)),
        r2_ss=dma((2,)),
        r2_rs=dma((2,)),
        b_ss=dma((2,)),
        b_rs=dma((2,)),
        c_ss=dma((4,)),
        c_rs=dma((4,)),
    )


def step_kernel(size, names, tok_in, sp, up_hbm, down_hbm, cot_in, mixed_out, dtok_out, dsp_out, *scratch):
    E, H, J, T, TP, S, D, FF = size
    X, C = H // 2, D // LANES
    half = J // 2
    v = types.SimpleNamespace(**dict(zip(names, scratch, strict=True)))
    ex = lax.axis_index("expert")
    hi = lax.axis_index("hidden")
    x, core = lax.div(hi, 2), lax.rem(hi, 2)

    def chip(dx):
        return lax.rem(x + dx + X, X)

    def at(dx, flip=0):
        return chip(dx) * 2 + (1 - core if flip else core)

    def copy(src, dst, ss, rs, e=None, h=None):
        return pltpu.make_async_remote_copy(
            src_ref=src,
            dst_ref=dst,
            send_sem=ss,
            recv_sem=rs,
            device_id={"expert": ex if e is None else e, "hidden": hi if h is None else h},
            device_id_type=MESH,
        )

    loads = [
        pltpu.make_async_copy(src, dst, v.in_sem.at[i])
        for i, (src, dst) in enumerate([(up_hbm, v.up), (down_hbm, v.down)])
    ]
    for load in loads:
        load.start()

    barrier = pltpu.get_barrier_semaphore()

    def greet_z(i, carry):
        pl.semaphore_signal(
            barrier, inc=1, device_id={"expert": lax.rem(ex + i, E), "hidden": hi}, device_id_type=MESH
        )
        return carry

    def greet_x(i, carry):
        pl.semaphore_signal(
            barrier, inc=1, device_id={"expert": ex, "hidden": lax.rem(hi + i, H)}, device_id_type=MESH
        )
        return carry

    lax.fori_loop(1, E, greet_z, 0)
    lax.fori_loop(1, H, greet_x, 0)

    def far_first(i):
        return E // 2 + (1 - 2 * lax.rem(i, 2)) * lax.div(i + 1, 2)

    def z_start(send, recv, ss, rs):
        def body(i, carry):
            peer = lax.rem(ex + far_first(i), E)
            copy(send.at[peer], recv.at[ex], ss, rs, e=peer).start()
            return carry

        lax.fori_loop(0, E - 1, body, 0)
        recv[ex] = send[ex]

    def landed(ref, sem):
        copy(ref, ref, sem, sem, h=at(0, 1)).wait_recv()

    def left(ref, sem):
        copy(ref, ref, sem, sem, h=at(0, 1)).wait_send()

    stage = v.stage

    def dispatch(k, value):
        for c in range(C):
            stage[c * S : (c + 1) * S, :] = value[:, c * LANES : (c + 1) * LANES]
        for e in range(E):
            rows = [stage[pl.ds(e * J + j, C, stride=S), :] for j in range(J)]
            v.a_send[k, e] = jnp.concatenate(rows, axis=0).astype(BF16)
        z_start(v.a_send.at[k], v.a_recv.at[k], v.a_ss.at[k], v.a_rs.at[k])

    lo, up = pl.ds(0, half), pl.ds(half, half)
    both = (lo, up)

    def pass_on(k, part, dx, to, sem):
        ref = v.g.at[k, both[part], at(dx)]
        copy(ref, ref, v.g_ss.at[k], v.g_rs.at[k, sem], h=to).start()

    def take(k, part, dx, sem):
        landed(v.g.at[k, both[part], at(dx)], v.g_rs.at[k, sem])
        pass_on(k, part, dx, at(0, 1), 6)

    def gather_start(k):
        landed(v.a_recv.at[k, pl.ds(0, E - 1)], v.a_rs.at[k])
        stage[...] = v.a_recv[k].reshape(E * J * C, LANES).astype(F32)
        for part in (0, 1):
            for j in range(part * half, (part + 1) * half):
                for c in range(C):
                    v.g[k, j, hi, :, c * LANES : (c + 1) * LANES] = stage[
                        pl.ds(j * C + c, E, stride=J * C), :
                    ].astype(BF16)
            pass_on(k, part, 0, at(1) if part == 0 else at(-1), 0 if part == 0 else 3)
        pass_on(k, 1, 0, at(1), 1)
        pass_on(k, 0, 0, at(-1), 2)
        for part in (0, 1):
            pass_on(k, part, 0, at(0, 1), 6)

    def gather_forward(k):
        take(k, 0, -1, 0)
        pass_on(k, 0, -1, at(1), 4)
        take(k, 1, 1, 3)
        pass_on(k, 1, 1, at(-1), 5)

    def gather_rest(k):
        take(k, 1, -1, 1)
        take(k, 0, 1, 2)

    def gather_far(k):
        take(k, 0, 2, 4)
        take(k, 1, 2, 5)

    def gather_finish(k):
        landed(v.g.at[k, :, pl.ds(0, X)], v.g_rs.at[k, 6])

    order = (2, 1, -1, 0)

    def d_copy(k, i, part):
        return copy(
            v.d_send.at[k, i, part], v.d_recv.at[k, i, part], v.d_ss.at[k], v.d_rs.at[k, i, part], h=at(0, 1)
        )

    def sum_start(k, part):
        for i, dx in enumerate(order):
            v.d_send[k, i, part] = v.part[k, both[part], at(dx, 1)].astype(BF16)
            d_copy(k, i, part).start()

    def chip_sum(k, i, part):
        return v.part[k, both[part], at(order[i])] + v.d_recv[k, i, part].astype(F32)

    def to_side(side):
        return at(1) if side == 0 else at(-1)

    def r2_send(k, side, part, value):
        v.r2_send[k, side, part] = value.astype(BF16)
        copy(
            v.r2_send.at[k, side, part], v.r2_recv.at[k, side, part], v.r2_ss.at[k], v.r2_rs.at[k], h=to_side(side)
        ).start()

    def sum_middle(k, part):
        d_copy(k, 0, part).wait_recv()
        v.r1_send[k, part] = chip_sum(k, 0, part).astype(BF16)
        copy(
            v.r1_send.at[k, part], v.r1_recv.at[k, part], v.r1_ss.at[k], v.r1_rs.at[k, part], h=to_side(part)
        ).start()
        near = 2 - part
        d_copy(k, near, part).wait_recv()
        r2_send(k, 1 - part, part, chip_sum(k, near, part))

    def sum_last(k, part):
        landed(v.r1_recv.at[k, part], v.r1_rs.at[k, part])
        near = 1 + part
        d_copy(k, near, part).wait_recv()
        r2_send(k, part, part, chip_sum(k, near, part) + v.r1_recv[k, part].astype(F32))

    def sum_return(k):
        for part in (0, 1):
            d_copy(k, 3, part).wait_recv()
        landed(v.r2_recv.at[k], v.r2_rs.at[k])
        for j in range(J):
            part, inner = divmod(j, half)
            total = v.part[k, j, at(0)] + v.d_recv[k, 3, part, inner].astype(F32)
            total = total + v.r2_recv[k, 0, part, inner].astype(F32) + v.r2_recv[k, 1, part, inner].astype(F32)
            for c in range(C):
                stage[pl.ds(j * C + c, E, stride=J * C), :] = total[:, c * LANES : (c + 1) * LANES]
        v.b_send[k] = stage[...].astype(BF16).reshape(E, J * C, LANES)
        z_start(v.b_send.at[k], v.b_recv.at[k], v.b_ss.at[k], v.b_rs.at[k])

    def collect(k):
        landed(v.b_recv.at[k, pl.ds(0, E - 1)], v.b_rs.at[k])
        stage[...] = v.b_recv[k].reshape(E * J * C, LANES).astype(F32)
        for c in range(C):
            v.slots[k, :, c * LANES : (c + 1) * LANES] = stage[pl.ds(c, S, stride=C), :].astype(BF16)

    tail = T - T % 16
    v.tok[tail:, :] = jnp.zeros((TP - tail, D), BF16)
    v.tok[:T, :] = tok_in[...]
    logits_t = dot(sp[...], v.tok[...], NT)
    held = lax.broadcasted_iota(jnp.int32, (S, TP), 1) < T
    masked = jnp.where(held, logits_t, -jnp.inf)
    raised = jnp.exp(masked - jnp.max(masked, axis=1, keepdims=True))
    disp_t = raised / jnp.sum(raised, axis=1, keepdims=True)
    v.disp_t[...] = disp_t
    slots_in = dot(disp_t.astype(BF16), v.tok[...])
    pl.semaphore_wait(barrier, E - 1 + H - 1)
    dispatch(0, slots_in)

    raised = jnp.exp(logits_t - jnp.max(logits_t, axis=0, keepdims=True))
    comb_t = raised / jnp.sum(raised, axis=0, keepdims=True)
    v.comb_t[...] = comb_t
    v.cot[tail:, :] = jnp.zeros((TP - tail, D), BF16)
    v.cot[:T, :] = cot_in[...]
    dispatch(1, dot(comb_t.astype(BF16), v.cot[...]))

    logits = dot(v.tok[...], sp[...], NT)
    held = lax.broadcasted_iota(jnp.int32, (TP, S), 0) < T
    masked = jnp.where(held, logits, -jnp.inf)
    raised = jnp.exp(masked - jnp.max(masked, axis=0, keepdims=True))
    v.disp[...] = raised / jnp.sum(raised, axis=0, keepdims=True)
    raised = jnp.exp(logits - jnp.max(logits, axis=1, keepdims=True))
    v.comb[...] = raised / jnp.sum(raised, axis=1, keepdims=True)

    def forward(j, carry):
        pre = dot(v.g[0, j].reshape(H * E, D), v.up[j])
        v.pre[j] = pre
        out = dot(gelu_exact(pre).astype(BF16), v.down[j])
        v.part[0, j] = out.reshape(H, E, D)
        return carry

    def slopes(j, carry):
        v.pre[j] = gelu_slope(v.pre[j])
        return carry

    def backward(j, carry):
        inward = dot(v.g[1, j].reshape(H * E, D), v.down[j], NT)
        d_pre = (inward * v.pre[j]).astype(BF16)
        v.part[1, j] = dot(d_pre, v.up[j], NT).reshape(H, E, D)
        return carry

    gather_start(0)
    gather_forward(0)
    gather_rest(0)
    gather_start(1)
    gather_far(0)
    gather_finish(0)
    for load in loads:
        load.wait()
    lax.fori_loop(0, half, forward, 0)
    gather_forward(1)
    sum_start(0, 0)
    lax.fori_loop(half, J, forward, 0)
    gather_rest(1)
    sum_start(0, 1)
    lax.fori_loop(0, J, slopes, 0)
    sum_middle(0, 0)
    sum_middle(0, 1)
    gather_far(1)
    gather_finish(1)
    lax.fori_loop(0, half, backward, 0)
    sum_start(1, 0)
    sum_last(0, 0)
    sum_last(0, 1)
    lax.fori_loop(half, J, backward, 0)
    sum_start(1, 1)
    sum_middle(1, 0)
    sum_middle(1, 1)
    sum_return(0)
    sum_last(1, 0)
    sum_last(1, 1)
    sum_return(1)

    collect(0)
    slots_out = v.slots[0]
    mixed = dot(v.comb[...].astype(BF16), slots_out)
    mixed_out[...] = mixed[:T].astype(BF16)
    comb_t = v.comb_t[...]
    d_comb = dot(slots_out, v.cot[...], NT)
    grad_ct = (comb_t * (d_comb - jnp.sum(comb_t * d_comb, axis=0, keepdims=True))).astype(BF16)
    v.dsp_c[...] = dot(grad_ct, v.tok[...])
    comb = v.comb[...]
    d_comb = dot(v.cot[...], slots_out, NT)
    v.grad_c[...] = (comb * (d_comb - jnp.sum(comb * d_comb, axis=1, keepdims=True))).astype(BF16)

    collect(1)
    d_slots = v.slots[1]
    disp_t = v.disp_t[...]
    d_disp = dot(d_slots, v.tok[...], NT)
    grad_dt = (disp_t * (d_disp - jnp.sum(disp_t * d_disp, axis=1, keepdims=True))).astype(BF16)
    grad = dot(grad_dt, v.tok[...]) + v.dsp_c[...]
    for h in range(H):
        block = grad[:, h * LANES : (h + 1) * LANES]
        v.c_own[h] = block
        v.c_send[h] = block.astype(BF16)

    def c_copy(slot):
        dx, flip = divmod(slot, 2)
        peer = at(dx, flip)
        return copy(v.c_send.at[peer], v.c_recv.at[slot], v.c_ss.at[0], v.c_rs.at[0], h=peer)

    row = (4, 5, 2, 3, 6, 7, 1)
    for slot in row:
        c_copy(slot).start()

    d_disp = dot(v.tok[...], d_slots, NT)
    disp = v.disp[...]
    grad_d = (disp * (d_disp - jnp.sum(disp * d_disp, axis=0, keepdims=True))).astype(BF16)
    d_tok = dot(disp.astype(BF16), d_slots) + dot(v.grad_c[...], sp[...]) + dot(grad_d, sp[...])
    dtok_out[...] = d_tok[:T].astype(BF16)

    total = v.c_own[hi]
    landed(v.c_recv.at[pl.ds(0, H - 1)], v.c_rs.at[0])
    for slot in row:
        total = total + v.c_recv[slot].astype(F32)

    place, base = lax.rem(ex, SPAN), lax.div(ex, SPAN)
    groups = E // SPAN
    near = total.astype(BF16)
    v.n_send[...] = near
    v.n_all[place] = near

    def n_copy(off):
        peer = base * SPAN + lax.rem(place + off, SPAN)
        return copy(v.n_send, v.n_all.at[place], v.c_ss.at[1], v.c_rs.at[1], e=peer)

    for off in range(1, SPAN):
        n_copy(off).start()
    landed(v.n_all.at[pl.ds(0, SPAN - 1)], v.c_rs.at[1])
    total = v.n_all[0].astype(F32)
    for i in range(1, SPAN):
        total = total + v.n_all[i].astype(F32)
    near = total.astype(BF16)
    v.w_send[...] = near
    v.w_all[base] = near

    def w_copy(off):
        peer = lax.rem(base + off, groups) * SPAN + place
        return copy(v.w_send, v.w_all.at[base], v.c_ss.at[2], v.c_rs.at[2], e=peer)

    far = sorted(range(1, groups), key=lambda off: -min(off, groups - off))
    for off in far:
        w_copy(off).start()
    landed(v.w_all.at[pl.ds(0, groups - 1)], v.c_rs.at[2])
    total = v.w_all[0].astype(F32)
    for i in range(1, groups):
        total = total + v.w_all[i].astype(F32)
    near = total.astype(BF16)
    v.f_send[...] = near
    v.f_all[hi] = near

    def f_copy(slot):
        dx, flip = divmod(slot, 2)
        return copy(v.f_send, v.f_all.at[hi], v.c_ss.at[3], v.c_rs.at[3], h=at(dx, flip))

    for slot in row:
        f_copy(slot).start()
    landed(v.f_all.at[pl.ds(0, H - 1)], v.c_rs.at[3])
    for h in range(H):
        dsp_out[:, h * LANES : (h + 1) * LANES] = v.f_all[h].astype(F32)

    for k in (0, 1):
        left(v.a_send.at[k, pl.ds(0, E - 1)], v.a_ss.at[k])
        left(v.b_send.at[k, pl.ds(0, E - 1)], v.b_ss.at[k])
        left(v.g.at[k, :, pl.ds(0, H - 1)], v.g_ss.at[k])
        left(v.d_send.at[k], v.d_ss.at[k])
        left(v.r1_send.at[k], v.r1_ss.at[k])
        left(v.r2_send.at[k], v.r2_ss.at[k])
    left(v.c_send.at[pl.ds(0, H - 1)], v.c_ss.at[0])
    left(v.n_all.at[pl.ds(0, SPAN - 1)], v.c_ss.at[1])
    left(v.w_all.at[pl.ds(0, groups - 1)], v.c_ss.at[2])
    left(v.f_all.at[pl.ds(0, H - 1)], v.c_ss.at[3])


def per_device(E, H, tokens, slot_params, expert_up, expert_down, cotangent):
    images, T, D = tokens.shape
    S = slot_params.shape[1]
    J, _, FF = expert_up.shape
    assert images == 1 and S == E * J and H == 8 and E % SPAN == 0 and D == H * LANES and J % 2 == 0
    size = (E, H, J, T, -(-T // LANES) * LANES, S, D, FF)
    plan = scratch_plan(*size)
    anywhere, local = pl.BlockSpec(memory_space=pl.ANY), pl.BlockSpec(memory_space=pltpu.VMEM)
    mixed, d_tokens, d_params = pl.pallas_call(
        functools.partial(step_kernel, size, tuple(plan)),
        out_shape=(
            jax.ShapeDtypeStruct((T, D), BF16),
            jax.ShapeDtypeStruct((T, D), BF16),
            jax.ShapeDtypeStruct((S, D), F32),
        ),
        in_specs=[local, local, anywhere, anywhere, local],
        out_specs=(local,) * 3,
        scratch_shapes=list(plan.values()),
        compiler_params=pltpu.CompilerParams(
            collective_id=0, has_side_effects=True, vmem_limit_bytes=52 * 1024 * 1024
        ),
    )(tokens.reshape(T, D), slot_params.T, expert_up, expert_down, cotangent.reshape(T, D))
    return mixed[None], d_tokens[None], d_params.T


def solution(mesh):
    own = P(("groups", "expert", "hidden"), None, None)
    return jax.shard_map(
        functools.partial(per_device, mesh.shape["expert"], mesh.shape["hidden"]),
        mesh=mesh,
        in_specs=(
            own,
            P("groups", None),
            P(("groups", "expert"), None, "hidden"),
            P(("groups", "expert"), "hidden", None),
            own,
        ),
        out_specs=(own, own, P("groups", None)),
        check_vma=False,
    )
```

```python
import functools
import types

import jax
import jax.numpy as jnp
from jax import lax
from jax.experimental import pallas as pl
from jax.experimental.pallas import tpu as pltpu
from jax.sharding import PartitionSpec as P

MESH = pl.DeviceIdType.MESH
BF16 = jnp.bfloat16
F32 = jnp.float32
LANES = 128
ROOT_HALF = 0.7071067811865476
ROOT_TAU = 0.3989422804014327
SPAN = 4

NT = (((1,), (1,)), ((), ()))
NN = (((1,), (0,)), ((), ()))


def dot(a, b, dims=NN):
    return lax.dot_general(a, b, dims, preferred_element_type=F32)


def gelu_exact(value):
    return 0.5 * value * (1.0 + lax.erf(value * ROOT_HALF))


def gelu_slope(value):
    return 0.5 * (1.0 + lax.erf(value * ROOT_HALF)) + value * jnp.exp(-0.5 * value * value) * ROOT_TAU


def scratch_plan(E, H, J, T, TP, S, D, FF):
    X, C = H // 2, D // LANES
    msg = J * C
    vm, dma = pltpu.VMEM, pltpu.SemaphoreType.DMA
    return dict(
        tok_in=vm((T, D), BF16),
        cot_in=vm((T, D), BF16),
        tok=vm((TP, D), BF16),
        cot=vm((TP, D), BF16),
        up=vm((J, D, FF), BF16),
        down=vm((J, FF, D), BF16),
        up_t=vm((J, FF, D), BF16),
        down_t=vm((J, D, FF), BF16),
        stage=vm((S * C, LANES), F32),
        a_send=vm((2, E, msg, LANES), BF16),
        a_recv=vm((2, E, msg, LANES), BF16),
        g=vm((2, J, H, E, D), BF16),
        pre=vm((J, H * E, FF), F32),
        part=vm((2, J, H, E, D), F32),
        d_send=vm((2, X, J, E, D), BF16),
        d_recv=vm((2, X, J, E, D), BF16),
        r1_send=vm((2, J, E, D), BF16),
        r1_recv=vm((2, J, E, D), BF16),
        r2_send=vm((2, 2, J, E, D), BF16),
        r2_recv=vm((2, 2, J, E, D), BF16),
        b_send=vm((2, 2, E, msg // 2, LANES), BF16),
        b_recv=vm((2, 2, E, msg // 2, LANES), BF16),
        slots=vm((2, S, D), BF16),
        comb=vm((TP, S), F32),
        comb_t=vm((S, TP), F32),
        disp=vm((TP, S), F32),
        disp_t=vm((S, TP), F32),
        grad_c=vm((TP, S), BF16),
        dsp_c=vm((S, D), F32),
        c_send=vm((H, S, LANES), BF16),
        c_own=vm((H, S, LANES), F32),
        c_recv=vm((H, S, LANES), BF16),
        n_all=vm((SPAN, S, LANES), BF16),
        n_send=vm((S, LANES), BF16),
        w_all=vm((E // SPAN, S, LANES), BF16),
        w_send=vm((S, LANES), BF16),
        f_all=vm((H, S, LANES), BF16),
        f_send=vm((S, LANES), BF16),
        in_sem=dma((4,)),
        a_ss=dma((2,)),
        a_rs=dma((2,)),
        g_ss=dma((2,)),
        g_rs=dma((2, 7)),
        d_ss=dma((2,)),
        d_rs=dma((2, X, J)),
        r1_ss=dma((2,)),
        r1_rs=dma((2, J)),
        r2_ss=dma((2,)),
        r2_rs=dma((2, 2)),
        b_ss=dma((2, 2)),
        b_rs=dma((2, 2)),
        c_ss=dma((4,)),
        c_rs=dma((4,)),
    )


def step_kernel(size, names, tok_hbm, sp, up_hbm, down_hbm, cot_hbm, mixed_out, dtok_out, dsp_out, *scratch):
    E, H, J, T, TP, S, D, FF = size
    X, C = H // 2, D // LANES
    half = J // 2
    v = types.SimpleNamespace(**dict(zip(names, scratch, strict=True)))
    ex = lax.axis_index("expert")
    hi = lax.axis_index("hidden")
    x, core = lax.div(hi, 2), lax.rem(hi, 2)

    def chip(dx):
        return lax.rem(x + dx + X, X)

    def at(dx, flip=0):
        return chip(dx) * 2 + (1 - core if flip else core)

    def copy(src, dst, ss, rs, e=None, h=None):
        return pltpu.make_async_remote_copy(
            src_ref=src,
            dst_ref=dst,
            send_sem=ss,
            recv_sem=rs,
            device_id={"expert": ex if e is None else e, "hidden": hi if h is None else h},
            device_id_type=MESH,
        )

    pairs = [(tok_hbm, v.tok_in), (cot_hbm, v.cot_in), (up_hbm, v.up), (down_hbm, v.down)]
    loads = [pltpu.make_async_copy(src, dst, v.in_sem.at[i]) for i, (src, dst) in enumerate(pairs)]
    for load in loads:
        load.start()

    barrier = pltpu.get_barrier_semaphore()

    def greet_z(i, carry):
        pl.semaphore_signal(
            barrier, inc=1, device_id={"expert": lax.rem(ex + i, E), "hidden": hi}, device_id_type=MESH
        )
        return carry

    def greet_x(i, carry):
        pl.semaphore_signal(
            barrier, inc=1, device_id={"expert": ex, "hidden": lax.rem(hi + i, H)}, device_id_type=MESH
        )
        return carry

    lax.fori_loop(1, E, greet_z, 0)
    lax.fori_loop(1, H, greet_x, 0)

    def far_first(i):
        return E // 2 + (1 - 2 * lax.rem(i, 2)) * lax.div(i + 1, 2)

    def z_start(send, recv, ss, rs):
        def body(i, carry):
            peer = lax.rem(ex + far_first(i), E)
            copy(send.at[peer], recv.at[ex], ss, rs, e=peer).start()
            return carry

        lax.fori_loop(0, E - 1, body, 0)
        recv[ex] = send[ex]

    def landed(ref, sem):
        copy(ref, ref, sem, sem, h=at(0, 1)).wait_recv()

    def left(ref, sem):
        copy(ref, ref, sem, sem, h=at(0, 1)).wait_send()

    stage = v.stage

    def dispatch(k, value):
        for c in range(C):
            stage[c * S : (c + 1) * S, :] = value[:, c * LANES : (c + 1) * LANES]
        for e in range(E):
            rows = [stage[pl.ds(e * J + j, C, stride=S), :] for j in range(J)]
            v.a_send[k, e] = jnp.concatenate(rows, axis=0).astype(BF16)
        z_start(v.a_send.at[k], v.a_recv.at[k], v.a_ss.at[k], v.a_rs.at[k])

    lo, up = pl.ds(0, half), pl.ds(half, half)
    both = (lo, up)

    def pass_on(k, part, dx, to, sem):
        ref = v.g.at[k, both[part], at(dx)]
        copy(ref, ref, v.g_ss.at[k], v.g_rs.at[k, sem], h=to).start()

    def take(k, part, dx, sem):
        landed(v.g.at[k, both[part], at(dx)], v.g_rs.at[k, sem])
        pass_on(k, part, dx, at(0, 1), 6)

    def gather_start(k):
        landed(v.a_recv.at[k, pl.ds(0, E - 1)], v.a_rs.at[k])
        stage[...] = v.a_recv[k].reshape(E * J * C, LANES).astype(F32)
        for part in (0, 1):
            for j in range(part * half, (part + 1) * half):
                for c in range(C):
                    v.g[k, j, hi, :, c * LANES : (c + 1) * LANES] = stage[
                        pl.ds(j * C + c, E, stride=J * C), :
                    ].astype(BF16)
            pass_on(k, part, 0, at(1) if part == 0 else at(-1), 0 if part == 0 else 3)
        pass_on(k, 1, 0, at(1), 1)
        pass_on(k, 0, 0, at(-1), 2)
        for part in (0, 1):
            pass_on(k, part, 0, at(0, 1), 6)

    def gather_forward(k):
        take(k, 0, -1, 0)
        pass_on(k, 0, -1, at(1), 4)
        take(k, 1, 1, 3)
        pass_on(k, 1, 1, at(-1), 5)

    def gather_rest(k):
        take(k, 1, -1, 1)
        take(k, 0, 1, 2)

    def gather_far(k):
        take(k, 0, 2, 4)
        take(k, 1, 2, 5)

    def gather_finish(k):
        landed(v.g.at[k, :, pl.ds(0, X)], v.g_rs.at[k, 6])

    order = (2, 1, -1, 0)

    def d_copy(k, i, j):
        return copy(v.d_send.at[k, i, j], v.d_recv.at[k, i, j], v.d_ss.at[k], v.d_rs.at[k, i, j], h=at(0, 1))

    def sum_start(k, j):
        for i, dx in enumerate(order):
            v.d_send[k, i, j] = v.part[k, j, at(dx, 1)].astype(BF16)
            d_copy(k, i, j).start()

    def chip_sum(k, i, j):
        d_copy(k, i, j).wait_recv()
        return v.part[k, j, at(order[i])] + v.d_recv[k, i, j].astype(F32)

    def to_side(side):
        return at(1) if side == 0 else at(-1)

    def r2_send(k, side, j, value):
        v.r2_send[k, side, j] = value.astype(BF16)
        copy(
            v.r2_send.at[k, side, j], v.r2_recv.at[k, side, j], v.r2_ss.at[k], v.r2_rs.at[k, j // half], h=to_side(side)
        ).start()

    def sum_middle(k, j):
        part = j // half
        v.r1_send[k, j] = chip_sum(k, 0, j).astype(BF16)
        copy(v.r1_send.at[k, j], v.r1_recv.at[k, j], v.r1_ss.at[k], v.r1_rs.at[k, j], h=to_side(part)).start()
        r2_send(k, 1 - part, j, chip_sum(k, 2 - part, j))

    def sum_last(k, j):
        part = j // half
        landed(v.r1_recv.at[k, j], v.r1_rs.at[k, j])
        r2_send(k, part, j, chip_sum(k, 1 + part, j) + v.r1_recv[k, j].astype(F32))

    def sum_return(k, part):
        landed(v.r2_recv.at[k, 0], v.r2_rs.at[k, part])
        rows = half * C
        for inner in range(half):
            j = part * half + inner
            total = chip_sum(k, 3, j) + v.r2_recv[k, 0, j].astype(F32) + v.r2_recv[k, 1, j].astype(F32)
            for c in range(C):
                stage[pl.ds(inner * C + c, E, stride=rows), :] = total[:, c * LANES : (c + 1) * LANES]
        v.b_send[k, part] = stage[: E * rows, :].astype(BF16).reshape(E, rows, LANES)
        z_start(v.b_send.at[k, part], v.b_recv.at[k, part], v.b_ss.at[k, part], v.b_rs.at[k, part])

    def collect(k):
        rows = half * C
        for part in (0, 1):
            landed(v.b_recv.at[k, part, pl.ds(0, E - 1)], v.b_rs.at[k, part])
            for e in range(E):
                at_row = (2 * e + part) * rows
                stage[at_row : at_row + rows, :] = v.b_recv[k, part, e].astype(F32)
        for c in range(C):
            v.slots[k, :, c * LANES : (c + 1) * LANES] = stage[pl.ds(c, S, stride=C), :].astype(BF16)

    loads[0].wait()
    tail = T - T % 16
    v.tok[tail:, :] = jnp.zeros((TP - tail, D), BF16)
    v.tok[:T, :] = v.tok_in[...]
    logits_t = dot(sp[...], v.tok[...], NT)
    held = lax.broadcasted_iota(jnp.int32, (S, TP), 1) < T
    masked = jnp.where(held, logits_t, -jnp.inf)
    raised = jnp.exp(masked - jnp.max(masked, axis=1, keepdims=True))
    disp_t = raised / jnp.sum(raised, axis=1, keepdims=True)
    v.disp_t[...] = disp_t
    slots_in = dot(disp_t.astype(BF16), v.tok[...])
    pl.semaphore_wait(barrier, E - 1 + H - 1)
    dispatch(0, slots_in)

    raised = jnp.exp(logits_t - jnp.max(logits_t, axis=0, keepdims=True))
    comb_t = raised / jnp.sum(raised, axis=0, keepdims=True)
    v.comb_t[...] = comb_t
    loads[1].wait()
    v.cot[tail:, :] = jnp.zeros((TP - tail, D), BF16)
    v.cot[:T, :] = v.cot_in[...]
    dispatch(1, dot(comb_t.astype(BF16), v.cot[...]))

    logits = dot(v.tok[...], sp[...], NT)
    held = lax.broadcasted_iota(jnp.int32, (TP, S), 0) < T
    masked = jnp.where(held, logits, -jnp.inf)
    raised = jnp.exp(masked - jnp.max(masked, axis=0, keepdims=True))
    v.disp[...] = raised / jnp.sum(raised, axis=0, keepdims=True)
    raised = jnp.exp(logits - jnp.max(logits, axis=1, keepdims=True))
    v.comb[...] = raised / jnp.sum(raised, axis=1, keepdims=True)

    for load in loads[2:]:
        load.wait()

    def turn(j, carry):
        v.up_t[j] = v.up[j].T
        v.down_t[j] = v.down[j].T
        return carry

    lax.fori_loop(0, J, turn, 0)

    def forward(j):
        pre = dot(v.g[0, j].reshape(H * E, D), v.up[j])
        v.pre[j] = pre
        out = dot(gelu_exact(pre).astype(BF16), v.down[j])
        v.part[0, j] = out.reshape(H, E, D)

    def slopes(j, carry):
        v.pre[j] = gelu_slope(v.pre[j])
        return carry

    def backward(j):
        inward = dot(v.g[1, j].reshape(H * E, D), v.down_t[j])
        d_pre = (inward * v.pre[j]).astype(BF16)
        v.part[1, j] = dot(d_pre, v.up_t[j]).reshape(H, E, D)

    turns = [j + part * half for j in range(half) for part in (0, 1)]
    gather_start(0)
    gather_forward(0)
    gather_rest(0)
    gather_start(1)
    gather_far(0)
    gather_finish(0)
    for i, j in enumerate(turns):
        forward(j)
        sum_start(0, j)
        if i == 1:
            gather_forward(1)
        if i > 0:
            sum_middle(0, turns[i - 1])
    gather_rest(1)
    lax.fori_loop(0, J, slopes, 0)
    sum_middle(0, turns[-1])
    gather_far(1)
    for j in turns[:2]:
        sum_last(0, j)
    gather_finish(1)
    for i, j in enumerate(turns):
        backward(j)
        sum_start(1, j)
        if i > 0:
            sum_middle(1, turns[i - 1])
        if i < 2:
            sum_last(0, turns[i + 2])
    for part in (0, 1):
        sum_return(0, part)
    sum_middle(1, turns[-1])
    for j in turns:
        sum_last(1, j)
    for part in (0, 1):
        sum_return(1, part)

    collect(0)
    slots_out = v.slots[0]
    mixed = dot(v.comb[...].astype(BF16), slots_out)
    mixed_out[...] = mixed[:T].astype(BF16)
    comb_t = v.comb_t[...]
    d_comb = dot(slots_out, v.cot[...], NT)
    grad_ct = (comb_t * (d_comb - jnp.sum(comb_t * d_comb, axis=0, keepdims=True))).astype(BF16)
    v.dsp_c[...] = dot(grad_ct, v.tok[...])
    comb = v.comb[...]
    d_comb = dot(v.cot[...], slots_out, NT)
    v.grad_c[...] = (comb * (d_comb - jnp.sum(comb * d_comb, axis=1, keepdims=True))).astype(BF16)

    collect(1)
    d_slots = v.slots[1]
    disp_t = v.disp_t[...]
    d_disp = dot(d_slots, v.tok[...], NT)
    grad_dt = (disp_t * (d_disp - jnp.sum(disp_t * d_disp, axis=1, keepdims=True))).astype(BF16)
    grad = dot(grad_dt, v.tok[...]) + v.dsp_c[...]
    for h in range(H):
        block = grad[:, h * LANES : (h + 1) * LANES]
        v.c_own[h] = block
        v.c_send[h] = block.astype(BF16)

    def c_copy(slot):
        dx, flip = divmod(slot, 2)
        peer = at(dx, flip)
        return copy(v.c_send.at[peer], v.c_recv.at[slot], v.c_ss.at[0], v.c_rs.at[0], h=peer)

    row = (4, 5, 2, 3, 6, 7, 1)
    for slot in row:
        c_copy(slot).start()

    d_disp = dot(v.tok[...], d_slots, NT)
    disp = v.disp[...]
    grad_d = (disp * (d_disp - jnp.sum(disp * d_disp, axis=0, keepdims=True))).astype(BF16)
    d_tok = dot(disp.astype(BF16), d_slots) + dot(v.grad_c[...], sp[...]) + dot(grad_d, sp[...])
    dtok_out[...] = d_tok[:T].astype(BF16)

    total = v.c_own[hi]
    landed(v.c_recv.at[pl.ds(0, H - 1)], v.c_rs.at[0])
    for slot in row:
        total = total + v.c_recv[slot].astype(F32)

    place, base = lax.rem(ex, SPAN), lax.div(ex, SPAN)
    groups = E // SPAN
    near = total.astype(BF16)
    v.n_send[...] = near
    v.n_all[place] = near

    def n_copy(off):
        peer = base * SPAN + lax.rem(place + off, SPAN)
        return copy(v.n_send, v.n_all.at[place], v.c_ss.at[1], v.c_rs.at[1], e=peer)

    for off in range(1, SPAN):
        n_copy(off).start()
    landed(v.n_all.at[pl.ds(0, SPAN - 1)], v.c_rs.at[1])
    total = v.n_all[0].astype(F32)
    for i in range(1, SPAN):
        total = total + v.n_all[i].astype(F32)
    near = total.astype(BF16)
    v.w_send[...] = near
    v.w_all[base] = near

    def w_copy(off):
        side = lax.rem(place + SPAN // 2, SPAN) if 2 * off == groups else place
        peer = lax.rem(base + off, groups) * SPAN + side
        return copy(v.w_send, v.w_all.at[base], v.c_ss.at[2], v.c_rs.at[2], e=peer)

    far = sorted(range(1, groups), key=lambda off: -min(off, groups - off))
    for off in far:
        w_copy(off).start()
    landed(v.w_all.at[pl.ds(0, groups - 1)], v.c_rs.at[2])
    total = v.w_all[0].astype(F32)
    for i in range(1, groups):
        total = total + v.w_all[i].astype(F32)
    near = total.astype(BF16)
    v.f_send[...] = near
    v.f_all[hi] = near

    def f_copy(slot):
        dx, flip = divmod(slot, 2)
        return copy(v.f_send, v.f_all.at[hi], v.c_ss.at[3], v.c_rs.at[3], h=at(dx, flip))

    for slot in row:
        f_copy(slot).start()
    landed(v.f_all.at[pl.ds(0, H - 1)], v.c_rs.at[3])
    for h in range(H):
        dsp_out[:, h * LANES : (h + 1) * LANES] = v.f_all[h].astype(F32)

    for k in (0, 1):
        left(v.a_send.at[k, pl.ds(0, E - 1)], v.a_ss.at[k])
        for part in (0, 1):
            left(v.b_send.at[k, part, pl.ds(0, E - 1)], v.b_ss.at[k, part])
        left(v.g.at[k, :, pl.ds(0, H - 1)], v.g_ss.at[k])
        left(v.d_send.at[k], v.d_ss.at[k])
        left(v.r1_send.at[k], v.r1_ss.at[k])
        left(v.r2_send.at[k], v.r2_ss.at[k])
    left(v.c_send.at[pl.ds(0, H - 1)], v.c_ss.at[0])
    left(v.n_all.at[pl.ds(0, SPAN - 1)], v.c_ss.at[1])
    left(v.w_all.at[pl.ds(0, groups - 1)], v.c_ss.at[2])
    left(v.f_all.at[pl.ds(0, H - 1)], v.c_ss.at[3])


def per_device(E, H, tokens, slot_params, expert_up, expert_down, cotangent):
    images, T, D = tokens.shape
    S = slot_params.shape[1]
    J, _, FF = expert_up.shape
    assert images == 1 and S == E * J and H == 8 and E % SPAN == 0 and D == H * LANES and J % 2 == 0
    size = (E, H, J, T, -(-T // LANES) * LANES, S, D, FF)
    plan = scratch_plan(*size)
    anywhere, local = pl.BlockSpec(memory_space=pl.ANY), pl.BlockSpec(memory_space=pltpu.VMEM)
    mixed, d_tokens, d_params = pl.pallas_call(
        functools.partial(step_kernel, size, tuple(plan)),
        out_shape=(
            jax.ShapeDtypeStruct((T, D), BF16),
            jax.ShapeDtypeStruct((T, D), BF16),
            jax.ShapeDtypeStruct((S, D), F32),
        ),
        in_specs=[anywhere, local, anywhere, anywhere, anywhere],
        out_specs=(local,) * 3,
        scratch_shapes=list(plan.values()),
        compiler_params=pltpu.CompilerParams(
            collective_id=0, has_side_effects=True, vmem_limit_bytes=54016 * 1024
        ),
    )(tokens.reshape(T, D), slot_params.T, expert_up, expert_down, cotangent.reshape(T, D))
    return mixed[None], d_tokens[None], d_params.T


def solution(mesh):
    own = P(("groups", "expert", "hidden"), None, None)
    return jax.shard_map(
        functools.partial(per_device, mesh.shape["expert"], mesh.shape["hidden"]),
        mesh=mesh,
        in_specs=(
            own,
            P("groups", None),
            P(("groups", "expert"), None, "hidden"),
            P(("groups", "expert"), "hidden", None),
            own,
        ),
        out_specs=(own, own, P("groups", None)),
        check_vma=False,
    )
```

```python
import functools
import types

import jax
import jax.numpy as jnp
from jax import lax
from jax.experimental import pallas as pl
from jax.experimental.pallas import tpu as pltpu
from jax.sharding import PartitionSpec as P

MESH = pl.DeviceIdType.MESH
BF16 = jnp.bfloat16
F32 = jnp.float32
LANES = 128
ROOT_HALF = 0.7071067811865476
ROOT_TAU = 0.3989422804014327
SPAN = 4

NT = (((1,), (1,)), ((), ()))
NN = (((1,), (0,)), ((), ()))


def dot(a, b, dims=NN):
    return lax.dot_general(a, b, dims, preferred_element_type=F32)


def gelu_exact(value):
    return 0.5 * value * (1.0 + lax.erf(value * ROOT_HALF))


def gelu_slope(value):
    return 0.5 * (1.0 + lax.erf(value * ROOT_HALF)) + value * jnp.exp(-0.5 * value * value) * ROOT_TAU


def scratch_plan(E, H, J, T, TP, S, D, FF):
    X, C = H // 2, D // LANES
    msg = J * C
    vm, dma = pltpu.VMEM, pltpu.SemaphoreType.DMA
    return dict(
        tok_in=vm((T, D), BF16),
        cot_in=vm((T, D), BF16),
        tok=vm((TP, D), BF16),
        cot=vm((TP, D), BF16),
        up=vm((J, D, FF), BF16),
        down=vm((J, FF, D), BF16),
        up_t=vm((J, FF, D), BF16),
        down_t=vm((J, D, FF), BF16),
        stage=vm((S * C, LANES), F32),
        a_send=vm((2, E, msg, LANES), BF16),
        a_recv=vm((2, E, msg, LANES), BF16),
        g=vm((2, J, H, E, D), BF16),
        pre=vm((J, H * E, FF), F32),
        part=vm((2, J, H, E, D), F32),
        d_send=vm((2, X, J, E, D), BF16),
        d_recv=vm((2, X, J, E, D), BF16),
        r1_send=vm((2, J, E, D), BF16),
        r1_recv=vm((2, J, E, D), BF16),
        r2_send=vm((2, 2, J, E, D), BF16),
        r2_recv=vm((2, 2, J, E, D), BF16),
        b_send=vm((2, 2, E, msg // 2, LANES), BF16),
        b_recv=vm((2, 2, E, msg // 2, LANES), BF16),
        slots=vm((2, S, D), BF16),
        comb=vm((TP, S), F32),
        comb_t=vm((S, TP), F32),
        disp=vm((TP, S), F32),
        disp_t=vm((S, TP), F32),
        grad_c=vm((TP, S), BF16),
        dsp_c=vm((S, D), F32),
        c_send=vm((H, S, LANES), BF16),
        c_own=vm((H, S, LANES), F32),
        c_recv=vm((H, S, LANES), BF16),
        n_all=vm((SPAN, S, LANES), BF16),
        n_send=vm((S, LANES), BF16),
        w_all=vm((E // SPAN, S, LANES), BF16),
        w_send=vm((S, LANES), BF16),
        f_all=vm((H, S, LANES), BF16),
        f_send=vm((S, LANES), BF16),
        in_sem=dma((4,)),
        a_ss=dma((2,)),
        a_rs=dma((2,)),
        g_ss=dma((2,)),
        g_rs=dma((2, 7)),
        d_ss=dma((2,)),
        d_rs=dma((2, X, J)),
        r1_ss=dma((2,)),
        r1_rs=dma((2, J)),
        r2_ss=dma((2,)),
        r2_rs=dma((2, 2)),
        b_ss=dma((2, 2)),
        b_rs=dma((2, 2)),
        c_ss=dma((4,)),
        c_rs=dma((4,)),
    )


def step_kernel(size, names, tok_hbm, sp, up_hbm, down_hbm, cot_hbm, mixed_out, dtok_out, dsp_out, *scratch):
    E, H, J, T, TP, S, D, FF = size
    X, C = H // 2, D // LANES
    half = J // 2
    v = types.SimpleNamespace(**dict(zip(names, scratch, strict=True)))
    ex = lax.axis_index("expert")
    hi = lax.axis_index("hidden")
    x, core = lax.div(hi, 2), lax.rem(hi, 2)

    def chip(dx):
        return lax.rem(x + dx + X, X)

    def at(dx, flip=0):
        return chip(dx) * 2 + (1 - core if flip else core)

    def copy(src, dst, ss, rs, e=None, h=None):
        return pltpu.make_async_remote_copy(
            src_ref=src,
            dst_ref=dst,
            send_sem=ss,
            recv_sem=rs,
            device_id={"expert": ex if e is None else e, "hidden": hi if h is None else h},
            device_id_type=MESH,
        )

    pairs = [(tok_hbm, v.tok_in), (cot_hbm, v.cot_in), (up_hbm, v.up), (down_hbm, v.down)]
    loads = [pltpu.make_async_copy(src, dst, v.in_sem.at[i]) for i, (src, dst) in enumerate(pairs)]
    for load in loads:
        load.start()

    barrier = pltpu.get_barrier_semaphore()

    def greet_z(i, carry):
        pl.semaphore_signal(
            barrier, inc=1, device_id={"expert": lax.rem(ex + i, E), "hidden": hi}, device_id_type=MESH
        )
        return carry

    def greet_x(i, carry):
        pl.semaphore_signal(
            barrier, inc=1, device_id={"expert": ex, "hidden": lax.rem(hi + i, H)}, device_id_type=MESH
        )
        return carry

    lax.fori_loop(1, E, greet_z, 0)
    lax.fori_loop(1, H, greet_x, 0)

    def far_first(i):
        return E // 2 + (1 - 2 * lax.rem(i, 2)) * lax.div(i + 1, 2)

    def z_start(send, recv, ss, rs):
        def body(i, carry):
            peer = lax.rem(ex + far_first(i), E)
            copy(send.at[peer], recv.at[ex], ss, rs, e=peer).start()
            return carry

        lax.fori_loop(0, E - 1, body, 0)
        recv[ex] = send[ex]

    def landed(ref, sem):
        copy(ref, ref, sem, sem, h=at(0, 1)).wait_recv()

    def left(ref, sem):
        copy(ref, ref, sem, sem, h=at(0, 1)).wait_send()

    stage = v.stage

    def pack(k, value):
        for c in range(C):
            stage[c * S : (c + 1) * S, :] = value[:, c * LANES : (c + 1) * LANES]
        for e in range(E):
            rows = [stage[pl.ds(e * J + j, C, stride=S), :] for j in range(J)]
            v.a_send[k, e] = jnp.concatenate(rows, axis=0).astype(BF16)

    def dispatch(k):
        z_start(v.a_send.at[k], v.a_recv.at[k], v.a_ss.at[k], v.a_rs.at[k])

    lo, up = pl.ds(0, half), pl.ds(half, half)
    both = (lo, up)

    def pass_on(k, part, dx, to, sem):
        ref = v.g.at[k, both[part], at(dx)]
        copy(ref, ref, v.g_ss.at[k], v.g_rs.at[k, sem], h=to).start()

    def take(k, part, dx, sem):
        landed(v.g.at[k, both[part], at(dx)], v.g_rs.at[k, sem])
        pass_on(k, part, dx, at(0, 1), 6)

    def gather_start(k):
        landed(v.a_recv.at[k, pl.ds(0, E - 1)], v.a_rs.at[k])
        stage[...] = v.a_recv[k].reshape(E * J * C, LANES).astype(F32)
        for part in (0, 1):
            for j in range(part * half, (part + 1) * half):
                for c in range(C):
                    v.g[k, j, hi, :, c * LANES : (c + 1) * LANES] = stage[
                        pl.ds(j * C + c, E, stride=J * C), :
                    ].astype(BF16)
            pass_on(k, part, 0, at(1) if part == 0 else at(-1), 0 if part == 0 else 3)
        pass_on(k, 1, 0, at(1), 1)
        pass_on(k, 0, 0, at(-1), 2)
        for part in (0, 1):
            pass_on(k, part, 0, at(0, 1), 6)

    def gather_forward(k):
        take(k, 0, -1, 0)
        pass_on(k, 0, -1, at(1), 4)
        take(k, 1, 1, 3)
        pass_on(k, 1, 1, at(-1), 5)

    def gather_rest(k):
        take(k, 1, -1, 1)
        take(k, 0, 1, 2)

    def gather_far(k):
        take(k, 0, 2, 4)
        take(k, 1, 2, 5)

    def gather_finish(k):
        landed(v.g.at[k, :, pl.ds(0, X)], v.g_rs.at[k, 6])

    order = (2, 1, -1, 0)

    def d_copy(k, i, j):
        return copy(v.d_send.at[k, i, j], v.d_recv.at[k, i, j], v.d_ss.at[k], v.d_rs.at[k, i, j], h=at(0, 1))

    def sum_start(k, j):
        for i, dx in enumerate(order):
            v.d_send[k, i, j] = v.part[k, j, at(dx, 1)].astype(BF16)
            d_copy(k, i, j).start()

    def chip_sum(k, i, j):
        d_copy(k, i, j).wait_recv()
        return v.part[k, j, at(order[i])] + v.d_recv[k, i, j].astype(F32)

    def to_side(side):
        return at(1) if side == 0 else at(-1)

    def r2_send(k, side, j, value):
        v.r2_send[k, side, j] = value.astype(BF16)
        copy(
            v.r2_send.at[k, side, j], v.r2_recv.at[k, side, j], v.r2_ss.at[k], v.r2_rs.at[k, j // half], h=to_side(side)
        ).start()

    def sum_middle(k, j):
        part = j // half
        v.r1_send[k, j] = chip_sum(k, 0, j).astype(BF16)
        copy(v.r1_send.at[k, j], v.r1_recv.at[k, j], v.r1_ss.at[k], v.r1_rs.at[k, j], h=to_side(part)).start()
        r2_send(k, 1 - part, j, chip_sum(k, 2 - part, j))

    def sum_last(k, j):
        part = j // half
        landed(v.r1_recv.at[k, j], v.r1_rs.at[k, j])
        r2_send(k, part, j, chip_sum(k, 1 + part, j) + v.r1_recv[k, j].astype(F32))

    def sum_return(k, part):
        landed(v.r2_recv.at[k, 0], v.r2_rs.at[k, part])
        rows = half * C
        for inner in range(half):
            j = part * half + inner
            total = chip_sum(k, 3, j) + v.r2_recv[k, 0, j].astype(F32) + v.r2_recv[k, 1, j].astype(F32)
            for c in range(C):
                stage[pl.ds(inner * C + c, E, stride=rows), :] = total[:, c * LANES : (c + 1) * LANES]
        v.b_send[k, part] = stage[: E * rows, :].astype(BF16).reshape(E, rows, LANES)
        z_start(v.b_send.at[k, part], v.b_recv.at[k, part], v.b_ss.at[k, part], v.b_rs.at[k, part])

    def collect(k):
        rows = half * C
        for part in (0, 1):
            landed(v.b_recv.at[k, part, pl.ds(0, E - 1)], v.b_rs.at[k, part])
            for e in range(E):
                at_row = (2 * e + part) * rows
                stage[at_row : at_row + rows, :] = v.b_recv[k, part, e].astype(F32)
        for c in range(C):
            v.slots[k, :, c * LANES : (c + 1) * LANES] = stage[pl.ds(c, S, stride=C), :].astype(BF16)

    loads[0].wait()
    tail = T - T % 16
    v.tok[tail:, :] = jnp.zeros((TP - tail, D), BF16)
    v.tok[:T, :] = v.tok_in[...]
    logits_t = dot(sp[...], v.tok[...], NT)
    held = lax.broadcasted_iota(jnp.int32, (S, TP), 1) < T
    masked = jnp.where(held, logits_t, -jnp.inf)
    raised = jnp.exp(masked - jnp.max(masked, axis=1, keepdims=True))
    disp_t = raised / jnp.sum(raised, axis=1, keepdims=True)
    v.disp_t[...] = disp_t
    slots_in = dot(disp_t.astype(BF16), v.tok[...])
    pack(0, slots_in)

    raised = jnp.exp(logits_t - jnp.max(logits_t, axis=0, keepdims=True))
    comb_t = raised / jnp.sum(raised, axis=0, keepdims=True)
    v.comb_t[...] = comb_t
    loads[1].wait()
    v.cot[tail:, :] = jnp.zeros((TP - tail, D), BF16)
    v.cot[:T, :] = v.cot_in[...]
    pack(1, dot(comb_t.astype(BF16), v.cot[...]))
    pl.semaphore_wait(barrier, E - 1 + H - 1)
    dispatch(0)
    dispatch(1)

    logits = dot(v.tok[...], sp[...], NT)
    held = lax.broadcasted_iota(jnp.int32, (TP, S), 0) < T
    masked = jnp.where(held, logits, -jnp.inf)
    raised = jnp.exp(masked - jnp.max(masked, axis=0, keepdims=True))
    v.disp[...] = raised / jnp.sum(raised, axis=0, keepdims=True)
    raised = jnp.exp(logits - jnp.max(logits, axis=1, keepdims=True))
    v.comb[...] = raised / jnp.sum(raised, axis=1, keepdims=True)

    for load in loads[2:]:
        load.wait()

    def turn(j, carry):
        v.up_t[j] = v.up[j].T
        v.down_t[j] = v.down[j].T
        return carry

    lax.fori_loop(0, J, turn, 0)

    def forward(j):
        pre = dot(v.g[0, j].reshape(H * E, D), v.up[j])
        v.pre[j] = pre
        out = dot(gelu_exact(pre).astype(BF16), v.down[j])
        v.part[0, j] = out.reshape(H, E, D)

    def slopes(j, carry):
        v.pre[j] = gelu_slope(v.pre[j])
        return carry

    def backward(j):
        inward = dot(v.g[1, j].reshape(H * E, D), v.down_t[j])
        d_pre = (inward * v.pre[j]).astype(BF16)
        v.part[1, j] = dot(d_pre, v.up_t[j]).reshape(H, E, D)

    turns = [j + part * half for j in range(half) for part in (0, 1)]
    gather_start(0)
    gather_forward(0)
    gather_rest(0)
    gather_start(1)
    gather_far(0)
    gather_finish(0)
    for i, j in enumerate(turns):
        forward(j)
        sum_start(0, j)
        if i == 1:
            gather_forward(1)
        if i == 2:
            gather_rest(1)
        if i > 0:
            sum_middle(0, turns[i - 1])
    lax.fori_loop(0, J, slopes, 0)
    sum_middle(0, turns[-1])
    gather_far(1)
    gather_finish(1)
    for i, j in enumerate(turns):
        backward(j)
        sum_start(1, j)
        if i > 0:
            sum_middle(1, turns[i - 1])
        for one in turns[2 * i : 2 * i + 2]:
            sum_last(0, one)
    sum_middle(1, turns[-1])
    sum_last(1, turns[0])
    sum_return(0, 0)
    sum_last(1, turns[1])
    sum_last(1, turns[2])
    sum_return(0, 1)
    sum_last(1, turns[3])
    for part in (0, 1):
        sum_return(1, part)

    collect(0)
    slots_out = v.slots[0]
    mixed = dot(v.comb[...].astype(BF16), slots_out)
    mixed_out[...] = mixed[:T].astype(BF16)
    comb_t = v.comb_t[...]
    d_comb = dot(slots_out, v.cot[...], NT)
    grad_ct = (comb_t * (d_comb - jnp.sum(comb_t * d_comb, axis=0, keepdims=True))).astype(BF16)
    v.dsp_c[...] = dot(grad_ct, v.tok[...])
    comb = v.comb[...]
    d_comb = dot(v.cot[...], slots_out, NT)
    v.grad_c[...] = (comb * (d_comb - jnp.sum(comb * d_comb, axis=1, keepdims=True))).astype(BF16)

    collect(1)
    d_slots = v.slots[1]
    disp_t = v.disp_t[...]
    d_disp = dot(d_slots, v.tok[...], NT)
    grad_dt = (disp_t * (d_disp - jnp.sum(disp_t * d_disp, axis=1, keepdims=True))).astype(BF16)
    grad = dot(grad_dt, v.tok[...]) + v.dsp_c[...]
    for h in range(H):
        block = grad[:, h * LANES : (h + 1) * LANES]
        v.c_own[h] = block
        v.c_send[h] = block.astype(BF16)

    def c_copy(slot):
        dx, flip = divmod(slot, 2)
        peer = at(dx, flip)
        return copy(v.c_send.at[peer], v.c_recv.at[slot], v.c_ss.at[0], v.c_rs.at[0], h=peer)

    row = (4, 5, 2, 3, 6, 7, 1)
    for slot in row:
        c_copy(slot).start()

    d_disp = dot(v.tok[...], d_slots, NT)
    disp = v.disp[...]
    grad_d = (disp * (d_disp - jnp.sum(disp * d_disp, axis=0, keepdims=True))).astype(BF16)
    d_tok = dot(disp.astype(BF16), d_slots) + dot(v.grad_c[...], sp[...]) + dot(grad_d, sp[...])
    dtok_out[...] = d_tok[:T].astype(BF16)

    total = v.c_own[hi]
    landed(v.c_recv.at[pl.ds(0, H - 1)], v.c_rs.at[0])
    for slot in row:
        total = total + v.c_recv[slot].astype(F32)

    place, base = lax.rem(ex, SPAN), lax.div(ex, SPAN)
    groups = E // SPAN
    near = total.astype(BF16)
    v.n_send[...] = near
    v.n_all[place] = near

    def n_copy(off):
        peer = base * SPAN + lax.rem(place + off, SPAN)
        return copy(v.n_send, v.n_all.at[place], v.c_ss.at[1], v.c_rs.at[1], e=peer)

    for off in range(1, SPAN):
        n_copy(off).start()
    landed(v.n_all.at[pl.ds(0, SPAN - 1)], v.c_rs.at[1])
    total = v.n_all[0].astype(F32)
    for i in range(1, SPAN):
        total = total + v.n_all[i].astype(F32)
    near = total.astype(BF16)
    v.w_send[...] = near
    v.w_all[base] = near

    def w_copy(off):
        side = lax.rem(place + SPAN // 2, SPAN) if 2 * off == groups else place
        peer = lax.rem(base + off, groups) * SPAN + side
        return copy(v.w_send, v.w_all.at[base], v.c_ss.at[2], v.c_rs.at[2], e=peer)

    far = sorted(range(1, groups), key=lambda off: -min(off, groups - off))
    for off in far:
        w_copy(off).start()
    landed(v.w_all.at[pl.ds(0, groups - 1)], v.c_rs.at[2])
    total = v.w_all[0].astype(F32)
    for i in range(1, groups):
        total = total + v.w_all[i].astype(F32)
    near = total.astype(BF16)
    v.f_send[...] = near
    v.f_all[hi] = near

    def f_copy(slot):
        dx, flip = divmod(slot, 2)
        return copy(v.f_send, v.f_all.at[hi], v.c_ss.at[3], v.c_rs.at[3], h=at(dx, flip))

    for slot in row:
        f_copy(slot).start()
    landed(v.f_all.at[pl.ds(0, H - 1)], v.c_rs.at[3])
    for h in range(H):
        dsp_out[:, h * LANES : (h + 1) * LANES] = v.f_all[h].astype(F32)

    for k in (0, 1):
        left(v.a_send.at[k, pl.ds(0, E - 1)], v.a_ss.at[k])
        for part in (0, 1):
            left(v.b_send.at[k, part, pl.ds(0, E - 1)], v.b_ss.at[k, part])
        left(v.g.at[k, :, pl.ds(0, H - 1)], v.g_ss.at[k])
        left(v.d_send.at[k], v.d_ss.at[k])
        left(v.r1_send.at[k], v.r1_ss.at[k])
        left(v.r2_send.at[k], v.r2_ss.at[k])
    left(v.c_send.at[pl.ds(0, H - 1)], v.c_ss.at[0])
    left(v.n_all.at[pl.ds(0, SPAN - 1)], v.c_ss.at[1])
    left(v.w_all.at[pl.ds(0, groups - 1)], v.c_ss.at[2])
    left(v.f_all.at[pl.ds(0, H - 1)], v.c_ss.at[3])


def store_kernel(*refs):
    count = len(refs) // 2
    sems = refs[-1]
    copies = [pltpu.make_async_copy(refs[i], refs[count + i], sems.at[i]) for i in range(count)]
    for one in copies:
        one.start()
    for one in copies:
        one.wait()


def per_device(E, H, tokens, slot_params, expert_up, expert_down, cotangent):
    images, T, D = tokens.shape
    S = slot_params.shape[1]
    J, _, FF = expert_up.shape
    assert images == 1 and S == E * J and H == 8 and E % SPAN == 0 and D == H * LANES and J % 2 == 0
    size = (E, H, J, T, -(-T // LANES) * LANES, S, D, FF)
    plan = scratch_plan(*size)
    anywhere, local = pl.BlockSpec(memory_space=pl.ANY), pl.BlockSpec(memory_space=pltpu.VMEM)
    shapes = (
        jax.ShapeDtypeStruct((T, D), BF16),
        jax.ShapeDtypeStruct((T, D), BF16),
        jax.ShapeDtypeStruct((S, D), F32),
    )
    results = pl.pallas_call(
        functools.partial(step_kernel, size, tuple(plan)),
        out_shape=shapes,
        in_specs=[anywhere, local, anywhere, anywhere, anywhere],
        out_specs=(local,) * 3,
        scratch_shapes=list(plan.values()),
        compiler_params=pltpu.CompilerParams(
            collective_id=0, has_side_effects=True, vmem_limit_bytes=54016 * 1024
        ),
    )(tokens.reshape(T, D), slot_params.T, expert_up, expert_down, cotangent.reshape(T, D))
    mixed, d_tokens, d_params = pl.pallas_call(
        store_kernel,
        out_shape=shapes,
        in_specs=[anywhere] * 3,
        out_specs=(anywhere,) * 3,
        scratch_shapes=[pltpu.SemaphoreType.DMA((3,))],
        compiler_params=pltpu.CompilerParams(vmem_limit_bytes=1024 * 1024),
    )(*results)
    return mixed[None], d_tokens[None], d_params.T


def solution(mesh):
    own = P(("groups", "expert", "hidden"), None, None)
    return jax.shard_map(
        functools.partial(per_device, mesh.shape["expert"], mesh.shape["hidden"]),
        mesh=mesh,
        in_specs=(
            own,
            P("groups", None),
            P(("groups", "expert"), None, "hidden"),
            P(("groups", "expert"), "hidden", None),
            own,
        ),
        out_specs=(own, own, P("groups", None)),
        check_vma=False,
    )
```

```python
import functools
import types

import jax
import jax.numpy as jnp
from jax import lax
from jax.experimental import pallas as pl
from jax.experimental.pallas import tpu as pltpu
from jax.sharding import PartitionSpec as P

MESH = pl.DeviceIdType.MESH
BF16 = jnp.bfloat16
F32 = jnp.float32
LANES = 128
ROOT_HALF = 0.7071067811865476
ROOT_TAU = 0.3989422804014327
SPAN = 4

NT = (((1,), (1,)), ((), ()))
NN = (((1,), (0,)), ((), ()))


def dot(a, b, dims=NN):
    return lax.dot_general(a, b, dims, preferred_element_type=F32)


def gelu_exact(value):
    return 0.5 * value * (1.0 + lax.erf(value * ROOT_HALF))


def gelu_slope(value):
    return 0.5 * (1.0 + lax.erf(value * ROOT_HALF)) + value * jnp.exp(-0.5 * value * value) * ROOT_TAU


def scratch_plan(E, H, J, T, TP, S, D, FF):
    X, C = H // 2, D // LANES
    msg = J * C
    vm, dma = pltpu.VMEM, pltpu.SemaphoreType.DMA
    return dict(
        tok_in=vm((T, D), BF16),
        cot_in=vm((T, D), BF16),
        tok=vm((TP, D), BF16),
        cot=vm((TP, D), BF16),
        up=vm((J, D, FF), BF16),
        down=vm((J, FF, D), BF16),
        up_t=vm((J, FF, D), BF16),
        down_t=vm((J, D, FF), BF16),
        stage=vm((S * C, LANES), F32),
        a_send=vm((2, E, msg, LANES), BF16),
        a_recv=vm((2, E, msg, LANES), BF16),
        g=vm((2, J, H, E, D), BF16),
        pre=vm((J, H * E, FF), F32),
        part=vm((2, J, H, E, D), F32),
        d_send=vm((2, X, J, E, D), BF16),
        d_recv=vm((2, X, J, E, D), BF16),
        r1_send=vm((2, J, E, D), BF16),
        r1_recv=vm((2, J, E, D), BF16),
        r2_send=vm((2, 2, J, E, D), BF16),
        r2_recv=vm((2, 2, J, E, D), BF16),
        b_send=vm((2, 2, E, msg // 2, LANES), BF16),
        b_recv=vm((2, 2, E, msg // 2, LANES), BF16),
        slots=vm((2, S, D), BF16),
        comb=vm((TP, S), F32),
        comb_t=vm((S, TP), F32),
        disp=vm((TP, S), F32),
        disp_t=vm((S, TP), F32),
        grad_c=vm((TP, S), BF16),
        dsp_c=vm((S, D), F32),
        c_send=vm((H, S, LANES), BF16),
        c_own=vm((H, S, LANES), F32),
        c_recv=vm((H, S, LANES), BF16),
        n_all=vm((SPAN, S, LANES), BF16),
        n_send=vm((S, LANES), BF16),
        w_all=vm((E // SPAN, S, LANES), BF16),
        w_send=vm((S, LANES), BF16),
        f_all=vm((H, S, LANES), BF16),
        f_send=vm((S, LANES), BF16),
        in_sem=dma((4,)),
        a_ss=dma((2,)),
        a_rs=dma((2,)),
        g_ss=dma((2,)),
        g_rs=dma((2, 7)),
        d_ss=dma((2,)),
        d_rs=dma((2, X, J)),
        r1_ss=dma((2,)),
        r1_rs=dma((2, J)),
        r2_ss=dma((2,)),
        r2_rs=dma((2, 2)),
        b_ss=dma((2, 2)),
        b_rs=dma((2, 2)),
        c_ss=dma((4,)),
        c_rs=dma((4,)),
    )


def step_kernel(size, names, tok_hbm, sp, up_hbm, down_hbm, cot_hbm, mixed_out, dtok_out, dsp_out, *scratch):
    E, H, J, T, TP, S, D, FF = size
    X, C = H // 2, D // LANES
    half = J // 2
    v = types.SimpleNamespace(**dict(zip(names, scratch, strict=True)))
    ex = lax.axis_index("expert")
    hi = lax.axis_index("hidden")
    x, core = lax.div(hi, 2), lax.rem(hi, 2)

    def chip(dx):
        return lax.rem(x + dx + X, X)

    def at(dx, flip=0):
        return chip(dx) * 2 + (1 - core if flip else core)

    def copy(src, dst, ss, rs, e=None, h=None):
        return pltpu.make_async_remote_copy(
            src_ref=src,
            dst_ref=dst,
            send_sem=ss,
            recv_sem=rs,
            device_id={"expert": ex if e is None else e, "hidden": hi if h is None else h},
            device_id_type=MESH,
        )

    pairs = [(tok_hbm, v.tok_in), (cot_hbm, v.cot_in), (up_hbm, v.up), (down_hbm, v.down)]
    loads = [pltpu.make_async_copy(src, dst, v.in_sem.at[i]) for i, (src, dst) in enumerate(pairs)]
    for load in loads:
        load.start()

    barrier = pltpu.get_barrier_semaphore()

    def greet_z(i, carry):
        pl.semaphore_signal(
            barrier, inc=1, device_id={"expert": lax.rem(ex + i, E), "hidden": hi}, device_id_type=MESH
        )
        return carry

    def greet_x(i, carry):
        pl.semaphore_signal(
            barrier, inc=1, device_id={"expert": ex, "hidden": lax.rem(hi + i, H)}, device_id_type=MESH
        )
        return carry

    lax.fori_loop(1, E, greet_z, 0)
    lax.fori_loop(1, H, greet_x, 0)

    def far_first(i):
        return E // 2 + (1 - 2 * lax.rem(i, 2)) * lax.div(i + 1, 2)

    def z_start(send, recv, ss, rs):
        def body(i, carry):
            peer = lax.rem(ex + far_first(i), E)
            copy(send.at[peer], recv.at[ex], ss, rs, e=peer).start()
            return carry

        lax.fori_loop(0, E - 1, body, 0)
        recv[ex] = send[ex]

    def landed(ref, sem):
        copy(ref, ref, sem, sem, h=at(0, 1)).wait_recv()

    def left(ref, sem):
        copy(ref, ref, sem, sem, h=at(0, 1)).wait_send()

    stage = v.stage

    def pack(k, value):
        for c in range(C):
            stage[c * S : (c + 1) * S, :] = value[:, c * LANES : (c + 1) * LANES]
        for e in range(E):
            rows = [stage[pl.ds(e * J + j, C, stride=S), :] for j in range(J)]
            v.a_send[k, e] = jnp.concatenate(rows, axis=0).astype(BF16)

    def dispatch(k):
        z_start(v.a_send.at[k], v.a_recv.at[k], v.a_ss.at[k], v.a_rs.at[k])

    lo, up = pl.ds(0, half), pl.ds(half, half)
    both = (lo, up)

    def pass_on(k, part, dx, to, sem):
        ref = v.g.at[k, both[part], at(dx)]
        copy(ref, ref, v.g_ss.at[k], v.g_rs.at[k, sem], h=to).start()

    def take(k, part, dx, sem):
        landed(v.g.at[k, both[part], at(dx)], v.g_rs.at[k, sem])
        pass_on(k, part, dx, at(0, 1), 6)

    def gather_start(k):
        landed(v.a_recv.at[k, pl.ds(0, E - 1)], v.a_rs.at[k])
        stage[...] = v.a_recv[k].reshape(E * J * C, LANES).astype(F32)
        for part in (0, 1):
            for j in range(part * half, (part + 1) * half):
                for c in range(C):
                    v.g[k, j, hi, :, c * LANES : (c + 1) * LANES] = stage[
                        pl.ds(j * C + c, E, stride=J * C), :
                    ].astype(BF16)
            pass_on(k, part, 0, at(1) if part == 0 else at(-1), 0 if part == 0 else 3)
        pass_on(k, 1, 0, at(1), 1)
        pass_on(k, 0, 0, at(-1), 2)
        for part in (0, 1):
            pass_on(k, part, 0, at(0, 1), 6)

    def gather_forward(k):
        take(k, 0, -1, 0)
        pass_on(k, 0, -1, at(1), 4)
        take(k, 1, 1, 3)
        pass_on(k, 1, 1, at(-1), 5)

    def gather_rest(k):
        take(k, 1, -1, 1)
        take(k, 0, 1, 2)

    def gather_far(k):
        take(k, 0, 2, 4)
        take(k, 1, 2, 5)

    def gather_finish(k):
        landed(v.g.at[k, :, pl.ds(0, X)], v.g_rs.at[k, 6])

    order = (2, 1, -1, 0)

    def d_copy(k, i, j):
        return copy(v.d_send.at[k, i, j], v.d_recv.at[k, i, j], v.d_ss.at[k], v.d_rs.at[k, i, j], h=at(0, 1))

    def sum_start(k, j):
        for i, dx in enumerate(order):
            v.d_send[k, i, j] = v.part[k, j, at(dx, 1)].astype(BF16)
            d_copy(k, i, j).start()

    def chip_sum(k, i, j):
        d_copy(k, i, j).wait_recv()
        return v.part[k, j, at(order[i])] + v.d_recv[k, i, j].astype(F32)

    def to_side(side):
        return at(1) if side == 0 else at(-1)

    def r2_send(k, side, j, value):
        v.r2_send[k, side, j] = value.astype(BF16)
        copy(
            v.r2_send.at[k, side, j], v.r2_recv.at[k, side, j], v.r2_ss.at[k], v.r2_rs.at[k, j // half], h=to_side(side)
        ).start()

    def sum_middle(k, j):
        part = j // half
        v.r1_send[k, j] = chip_sum(k, 0, j).astype(BF16)
        copy(v.r1_send.at[k, j], v.r1_recv.at[k, j], v.r1_ss.at[k], v.r1_rs.at[k, j], h=to_side(part)).start()
        r2_send(k, 1 - part, j, chip_sum(k, 2 - part, j))

    def sum_last(k, j):
        part = j // half
        landed(v.r1_recv.at[k, j], v.r1_rs.at[k, j])
        r2_send(k, part, j, chip_sum(k, 1 + part, j) + v.r1_recv[k, j].astype(F32))

    def sum_return(k, part):
        landed(v.r2_recv.at[k, 0], v.r2_rs.at[k, part])
        rows = half * C
        for inner in range(half):
            j = part * half + inner
            total = chip_sum(k, 3, j) + v.r2_recv[k, 0, j].astype(F32) + v.r2_recv[k, 1, j].astype(F32)
            for c in range(C):
                stage[pl.ds(inner * C + c, E, stride=rows), :] = total[:, c * LANES : (c + 1) * LANES]
        v.b_send[k, part] = stage[: E * rows, :].astype(BF16).reshape(E, rows, LANES)
        z_start(v.b_send.at[k, part], v.b_recv.at[k, part], v.b_ss.at[k, part], v.b_rs.at[k, part])

    def collect(k):
        rows = half * C
        for part in (0, 1):
            landed(v.b_recv.at[k, part, pl.ds(0, E - 1)], v.b_rs.at[k, part])
            for e in range(E):
                at_row = (2 * e + part) * rows
                stage[at_row : at_row + rows, :] = v.b_recv[k, part, e].astype(F32)
        for c in range(C):
            v.slots[k, :, c * LANES : (c + 1) * LANES] = stage[pl.ds(c, S, stride=C), :].astype(BF16)

    loads[0].wait()
    tail = T - T % 16
    v.tok[tail:, :] = jnp.zeros((TP - tail, D), BF16)
    v.tok[:T, :] = v.tok_in[...]
    logits_t = dot(sp[...], v.tok[...], NT)
    held = lax.broadcasted_iota(jnp.int32, (S, TP), 1) < T
    masked = jnp.where(held, logits_t, -jnp.inf)
    raised = jnp.exp(masked - jnp.max(masked, axis=1, keepdims=True))
    disp_t = raised / jnp.sum(raised, axis=1, keepdims=True)
    v.disp_t[...] = disp_t
    slots_in = dot(disp_t.astype(BF16), v.tok[...])
    pack(0, slots_in)

    raised = jnp.exp(logits_t - jnp.max(logits_t, axis=0, keepdims=True))
    comb_t = raised / jnp.sum(raised, axis=0, keepdims=True)
    v.comb_t[...] = comb_t
    loads[1].wait()
    v.cot[tail:, :] = jnp.zeros((TP - tail, D), BF16)
    v.cot[:T, :] = v.cot_in[...]
    pack(1, dot(comb_t.astype(BF16), v.cot[...]))
    pl.semaphore_wait(barrier, E - 1 + H - 1)
    dispatch(0)
    dispatch(1)

    logits = dot(v.tok[...], sp[...], NT)
    held = lax.broadcasted_iota(jnp.int32, (TP, S), 0) < T
    masked = jnp.where(held, logits, -jnp.inf)
    raised = jnp.exp(masked - jnp.max(masked, axis=0, keepdims=True))
    v.disp[...] = raised / jnp.sum(raised, axis=0, keepdims=True)
    raised = jnp.exp(logits - jnp.max(logits, axis=1, keepdims=True))
    v.comb[...] = raised / jnp.sum(raised, axis=1, keepdims=True)

    for load in loads[2:]:
        load.wait()

    def turn(j, carry):
        v.up_t[j] = v.up[j].T
        v.down_t[j] = v.down[j].T
        return carry

    lax.fori_loop(0, J, turn, 0)

    def forward(j):
        pre = dot(v.g[0, j].reshape(H * E, D), v.up[j])
        v.pre[j] = pre
        out = dot(gelu_exact(pre).astype(BF16), v.down[j])
        v.part[0, j] = out.reshape(H, E, D)

    def slopes(j, carry):
        v.pre[j] = gelu_slope(v.pre[j])
        return carry

    def backward(j):
        inward = dot(v.g[1, j].reshape(H * E, D), v.down_t[j])
        d_pre = (inward * v.pre[j]).astype(BF16)
        v.part[1, j] = dot(d_pre, v.up_t[j]).reshape(H, E, D)

    turns = [j + part * half for j in range(half) for part in (0, 1)]
    gather_start(0)
    gather_forward(0)
    gather_rest(0)
    gather_start(1)
    gather_far(0)
    gather_finish(0)
    for i, j in enumerate(turns):
        forward(j)
        sum_start(0, j)
        if i == 1:
            gather_forward(1)
        if i > 0:
            sum_middle(0, turns[i - 1])
    gather_rest(1)
    lax.fori_loop(0, J, slopes, 0)
    sum_middle(0, turns[-1])
    gather_far(1)
    for j in turns[:2]:
        sum_last(0, j)
    gather_finish(1)
    for i, j in enumerate(turns):
        backward(j)
        sum_start(1, j)
        if i > 0:
            sum_middle(1, turns[i - 1])
        if i < 2:
            sum_last(0, turns[i + 2])
    for part in (0, 1):
        sum_return(0, part)
    sum_middle(1, turns[-1])
    for j in turns:
        sum_last(1, j)
    for part in (0, 1):
        sum_return(1, part)

    collect(0)
    slots_out = v.slots[0]
    mixed = dot(v.comb[...].astype(BF16), slots_out)
    mixed_out[...] = mixed[:T].astype(BF16)
    comb_t = v.comb_t[...]
    d_comb = dot(slots_out, v.cot[...], NT)
    grad_ct = (comb_t * (d_comb - jnp.sum(comb_t * d_comb, axis=0, keepdims=True))).astype(BF16)
    v.dsp_c[...] = dot(grad_ct, v.tok[...])
    comb = v.comb[...]
    d_comb = dot(v.cot[...], slots_out, NT)
    v.grad_c[...] = (comb * (d_comb - jnp.sum(comb * d_comb, axis=1, keepdims=True))).astype(BF16)

    collect(1)
    d_slots = v.slots[1]
    disp_t = v.disp_t[...]
    d_disp = dot(d_slots, v.tok[...], NT)
    grad_dt = (disp_t * (d_disp - jnp.sum(disp_t * d_disp, axis=1, keepdims=True))).astype(BF16)
    grad = dot(grad_dt, v.tok[...]) + v.dsp_c[...]
    for h in range(H):
        block = grad[:, h * LANES : (h + 1) * LANES]
        v.c_own[h] = block
        v.c_send[h] = block.astype(BF16)

    def c_copy(slot):
        dx, flip = divmod(slot, 2)
        peer = at(dx, flip)
        return copy(v.c_send.at[peer], v.c_recv.at[slot], v.c_ss.at[0], v.c_rs.at[0], h=peer)

    row = (4, 5, 2, 3, 6, 7, 1)
    for slot in row:
        c_copy(slot).start()

    d_disp = dot(v.tok[...], d_slots, NT)
    disp = v.disp[...]
    grad_d = (disp * (d_disp - jnp.sum(disp * d_disp, axis=0, keepdims=True))).astype(BF16)
    d_tok = dot(disp.astype(BF16), d_slots) + dot(v.grad_c[...], sp[...]) + dot(grad_d, sp[...])
    dtok_out[...] = d_tok[:T].astype(BF16)

    total = v.c_own[hi]
    landed(v.c_recv.at[pl.ds(0, H - 1)], v.c_rs.at[0])
    for slot in row:
        total = total + v.c_recv[slot].astype(F32)

    place, base = lax.rem(ex, SPAN), lax.div(ex, SPAN)
    groups = E // SPAN
    near = total.astype(BF16)
    v.n_send[...] = near
    v.n_all[place] = near

    def n_copy(off):
        peer = base * SPAN + lax.rem(place + off, SPAN)
        return copy(v.n_send, v.n_all.at[place], v.c_ss.at[1], v.c_rs.at[1], e=peer)

    for off in range(1, SPAN):
        n_copy(off).start()
    landed(v.n_all.at[pl.ds(0, SPAN - 1)], v.c_rs.at[1])
    total = v.n_all[0].astype(F32)
    for i in range(1, SPAN):
        total = total + v.n_all[i].astype(F32)
    near = total.astype(BF16)
    v.w_send[...] = near
    v.w_all[base] = near

    def w_copy(off):
        side = lax.rem(place + SPAN // 2, SPAN) if 2 * off == groups else place
        peer = lax.rem(base + off, groups) * SPAN + side
        return copy(v.w_send, v.w_all.at[base], v.c_ss.at[2], v.c_rs.at[2], e=peer)

    far = sorted(range(1, groups), key=lambda off: -min(off, groups - off))
    for off in far:
        w_copy(off).start()
    landed(v.w_all.at[pl.ds(0, groups - 1)], v.c_rs.at[2])
    total = v.w_all[0].astype(F32)
    for i in range(1, groups):
        total = total + v.w_all[i].astype(F32)
    near = total.astype(BF16)
    v.f_send[...] = near
    v.f_all[hi] = near

    def f_copy(slot):
        dx, flip = divmod(slot, 2)
        return copy(v.f_send, v.f_all.at[hi], v.c_ss.at[3], v.c_rs.at[3], h=at(dx, flip))

    for slot in row:
        f_copy(slot).start()
    landed(v.f_all.at[pl.ds(0, H - 1)], v.c_rs.at[3])
    for h in range(H):
        dsp_out[:, h * LANES : (h + 1) * LANES] = v.f_all[h].astype(F32)

    for k in (0, 1):
        left(v.a_send.at[k, pl.ds(0, E - 1)], v.a_ss.at[k])
        for part in (0, 1):
            left(v.b_send.at[k, part, pl.ds(0, E - 1)], v.b_ss.at[k, part])
        left(v.g.at[k, :, pl.ds(0, H - 1)], v.g_ss.at[k])
        left(v.d_send.at[k], v.d_ss.at[k])
        left(v.r1_send.at[k], v.r1_ss.at[k])
        left(v.r2_send.at[k], v.r2_ss.at[k])
    left(v.c_send.at[pl.ds(0, H - 1)], v.c_ss.at[0])
    left(v.n_all.at[pl.ds(0, SPAN - 1)], v.c_ss.at[1])
    left(v.w_all.at[pl.ds(0, groups - 1)], v.c_ss.at[2])
    left(v.f_all.at[pl.ds(0, H - 1)], v.c_ss.at[3])


def store_kernel(*refs):
    count = len(refs) // 2
    sems = refs[-1]
    copies = [pltpu.make_async_copy(refs[i], refs[count + i], sems.at[i]) for i in range(count)]
    for one in copies:
        one.start()
    for one in copies:
        one.wait()


def per_device(E, H, tokens, slot_params, expert_up, expert_down, cotangent):
    images, T, D = tokens.shape
    S = slot_params.shape[1]
    J, _, FF = expert_up.shape
    assert images == 1 and S == E * J and H == 8 and E % SPAN == 0 and D == H * LANES and J % 2 == 0
    size = (E, H, J, T, -(-T // LANES) * LANES, S, D, FF)
    plan = scratch_plan(*size)
    anywhere, local = pl.BlockSpec(memory_space=pl.ANY), pl.BlockSpec(memory_space=pltpu.VMEM)
    shapes = (
        jax.ShapeDtypeStruct((T, D), BF16),
        jax.ShapeDtypeStruct((T, D), BF16),
        jax.ShapeDtypeStruct((S, D), F32),
    )
    results = pl.pallas_call(
        functools.partial(step_kernel, size, tuple(plan)),
        out_shape=shapes,
        in_specs=[anywhere, local, anywhere, anywhere, anywhere],
        out_specs=(local,) * 3,
        scratch_shapes=list(plan.values()),
        compiler_params=pltpu.CompilerParams(
            collective_id=0, has_side_effects=True, vmem_limit_bytes=54016 * 1024
        ),
    )(tokens.reshape(T, D), slot_params.T, expert_up, expert_down, cotangent.reshape(T, D))
    mixed, d_tokens, d_params = pl.pallas_call(
        store_kernel,
        out_shape=shapes,
        in_specs=[anywhere] * 3,
        out_specs=(anywhere,) * 3,
        scratch_shapes=[pltpu.SemaphoreType.DMA((3,))],
        compiler_params=pltpu.CompilerParams(vmem_limit_bytes=1024 * 1024),
    )(*results)
    return mixed[None], d_tokens[None], d_params.T


def solution(mesh):
    own = P(("groups", "expert", "hidden"), None, None)
    return jax.shard_map(
        functools.partial(per_device, mesh.shape["expert"], mesh.shape["hidden"]),
        mesh=mesh,
        in_specs=(
            own,
            P("groups", None),
            P(("groups", "expert"), None, "hidden"),
            P(("groups", "expert"), "hidden", None),
            own,
        ),
        out_specs=(own, own, P("groups", None)),
        check_vma=False,
    )
```
